32 devices in a mesh: chan: 16 (over z, y, core), wall: 2 (over x).
Axes of the slice: x: 2, y: 2, z: 4, core: 2. Of those that a mesh axis runs over, the one named last changes fastest.
Arguments:
- coords: float32 [3, 16, 2, 4096], P(None, 'chan', 'wall'), as said below
- masses: float32 [16, 2, 4096], P('chan', 'wall'), may hold values from 0.5 to 2
- counts: int32 [16, 2, 16], P('chan', 'wall'), may hold values from 64 to 256
- lists: int32 [16, 2, 5, 16, 2], P('chan', 'wall'), may hold values from 0 to 47, as said below
Outputs:
- density: float32 [16, 2, 4096], P('chan', 'wall')
The draws below stay inside these ranges and needn't reach their ends.
Inputs may be any that keep to these rules, and one draw needn't show every extreme that they name: `lists`: each row of 2 entries names different tiles; tile t of extended slab s is s * 16 + t, slab 0 the lower cross-wall neighbour, 1 the slab itself, 2 the upper neighbour. `coords`: channel components lie in [0, 1), cross-wall and depth components in [0, 8).
All inputs are finite; a program needn't handle non-finite values.
Results may differ from the reference program's by a relative error of at most 0.0003.
Values sent between devices are 32-bit elements; how exact they have to be, the bound alone decides.
A program may use at most 64 MiB of HBM per device.

```python
import math
import jax
import jax.numpy as jnp
from jax import lax

TILE = 256
TILE_DEV = 16
NB = 2
R = 4
CHAN_SLABS = 16
WALL_SLABS = 2
PART = 4096


def draw_coords(key, part):
    unit = jax.random.uniform(key, (3, CHAN_SLABS, WALL_SLABS, TILE_DEV * TILE), jnp.float32)
    extent = jnp.array([1.0, 2.0 * R, 2.0 * R], jnp.float32).reshape(3, 1, 1, 1)
    return (unit * extent * 0.9999).astype(jnp.float32)


def draw_lists(key, part):
    choices_count = 3 * TILE_DEV
    scores = jax.random.randint(key, (CHAN_SLABS, WALL_SLABS, R + 1, TILE_DEV, choices_count), 0, 1 << 20, dtype=jnp.int32)
    distinct = scores * choices_count + jnp.arange(choices_count, dtype=jnp.int32)
    return jnp.argsort(distinct, axis=-1)[..., :NB].astype(jnp.int32)


def with_ends(drawn, own_key, low, top_value):
    spot = [jax.random.randint(jax.random.fold_in(own_key, axis), (), 0, length) for axis, length in enumerate(drawn.shape)]
    main_axis = drawn.shape.index(max(drawn.shape))
    neighbour = spot[:main_axis] + [(spot[main_axis] + 1) % drawn.shape[main_axis]] + spot[main_axis + 1:]
    return drawn.at[tuple(spot)].set(low).at[tuple(neighbour)].set(top_value)


def level_of(stream_key, dims, cuts, smallest, top_value):
    gain, own = 1.0, jax.random.fold_in(stream_key, 6)
    for axis_at, shards_of in cuts:
        draws = jnp.exp(jax.random.uniform(jax.random.fold_in(own, axis_at), (shards_of,), jnp.float32, smallest / len(cuts), top_value / len(cuts)))
        gain = gain * jnp.repeat(draws, dims[axis_at] // shards_of).reshape([-1 if axis == axis_at else 1 for axis in range(len(dims))])
    return gain


def setup_inputs(seed: int = 0) -> dict:
    streams_of = jax.random.split(jax.random.key(seed), 5)
    coords = draw_coords(jax.random.fold_in(streams_of[4], 71), 0)
    masses = jnp.clip(jnp.exp(math.log(2.0) - 1.3862944 * jax.random.uniform(streams_of[1], (CHAN_SLABS, WALL_SLABS, PART), jnp.float32) ** level_of(streams_of[1], (CHAN_SLABS, WALL_SLABS, PART), ((0, 16), (1, 2)), -0.2, 0.2)), 0.5, 2.0)
    counts = with_ends(jax.random.randint(streams_of[2], (CHAN_SLABS, WALL_SLABS, TILE_DEV), TILE // 4, TILE + 1), jax.random.fold_in(streams_of[2], 1), TILE // 4, TILE).astype(jnp.int32)
    lists = draw_lists(jax.random.fold_in(streams_of[4], 71), 0)
    return dict(coords=coords, masses=masses, counts=counts, lists=lists)


def spline(scaled):
    return (jnp.maximum(2.0 - scaled, 0.0) ** 3 * 0.25 - jnp.maximum(1.0 - scaled, 0.0) ** 3) * (1.0 / math.pi)

def pair_block(own_block, partner, partner_rows, offset):
    tile_count = own_block.shape[1]
    tile_len = own_block.shape[2]
    list_len = partner_rows.shape[1]
    picked = jnp.take(partner, partner_rows.reshape(-1), axis=1).reshape(4, tile_count, list_len, tile_len)
    wall_lift = (partner_rows // tile_count - 1).astype(jnp.float32) * (2.0 * R)
    reach = float(R)

    def single_tile(inputs):
        own_tile, theirs, shift_y = inputs
        delta_x = own_tile[0][None, :, None] - (theirs[0][:, None, :] + offset)
        delta_y = own_tile[1][None, :, None] - (theirs[1][:, None, :] + shift_y[:, None, None])
        delta_z = own_tile[2][None, :, None] - theirs[2][:, None, :]
        distance = jnp.sqrt(delta_x * delta_x + delta_y * delta_y + delta_z * delta_z + 0.0001)
        weight = spline(distance / reach)
        gained = lax.optimization_barrier(jnp.sum(weight * theirs[3][:, None, :], axis=(0, 2)))
        handed = lax.optimization_barrier(jnp.sum(weight * own_tile[3][None, :, None], axis=1))
        return (gained, handed)
    gained, handed = lax.map(single_tile, (jnp.moveaxis(own_block, 1, 0), jnp.moveaxis(picked, 1, 0), wall_lift))
    onehot = (partner_rows.reshape(-1)[:, None] == jnp.arange(partner.shape[1], dtype=jnp.int32)[None, :]).astype(jnp.float32)
    returned = jnp.dot(onehot.T, handed.reshape(-1, tile_len), precision=lax.Precision.HIGHEST)
    return (gained, returned)

def reference(coords, masses, counts, lists):
    tile_count = counts.shape[2]
    tile_len = masses.shape[2] // tile_count
    slots = jnp.arange(tile_len, dtype=jnp.int32)
    filled = (slots[None, None, None, :] < counts[..., None]).astype(jnp.float32)
    weighted = masses.reshape(filled.shape) * filled
    packed = jnp.concatenate([coords.reshape(3, CHAN_SLABS, WALL_SLABS, tile_count, tile_len), weighted[None]], axis=0)
    padded = jnp.pad(packed, ((0, 0), (0, 0), (1, 1), (0, 0), (0, 0)))
    extended = jnp.concatenate([padded[:, :, 0:WALL_SLABS], padded[:, :, 1:WALL_SLABS + 1], padded[:, :, 2:]], axis=3)
    flat_own = jnp.moveaxis(packed.reshape(4, -1, tile_count, tile_len), 1, 0)
    density = jnp.zeros((CHAN_SLABS, WALL_SLABS, tile_count, tile_len), jnp.float32)
    returns = jnp.zeros((CHAN_SLABS, WALL_SLABS, 3 * tile_count, tile_len), jnp.float32)
    for step in range(R + 1):
        partner = jnp.roll(extended, -step, axis=1)
        flat_partner = jnp.moveaxis(partner.reshape(4, -1, 3 * tile_count, tile_len), 1, 0)
        flat_lists = lists[:, :, step].reshape(-1, tile_count, NB)

        def per_device(inputs, offset=float(step)):
            return pair_block(inputs[0], inputs[1], inputs[2], offset)
        gained, handed = lax.map(per_device, (flat_own, flat_partner, flat_lists))
        density = density + gained.reshape(CHAN_SLABS, WALL_SLABS, tile_count, tile_len)
        if step > 0:
            returns = returns + jnp.roll(handed.reshape(CHAN_SLABS, WALL_SLABS, 3 * tile_count, tile_len), step, axis=0)
    lower = returns[:, :, :tile_count]
    center = returns[:, :, tile_count:2 * tile_count]
    upper = returns[:, :, 2 * tile_count:]
    from_below = jnp.pad(upper, ((0, 0), (1, 0), (0, 0), (0, 0)))[:, :WALL_SLABS]
    from_above = jnp.pad(lower, ((0, 0), (0, 1), (0, 0), (0, 0)))[:, 1:]
    total = density + center + from_below + from_above
    return (total * filled / (NB * tile_len)).reshape(CHAN_SLABS, WALL_SLABS, -1)
```

```python
import functools
import math

import jax
import jax.numpy as jnp
from jax import lax
from jax.experimental import pallas as pl
from jax.experimental.pallas import tpu as pltpu
from jax.sharding import PartitionSpec as P

NB = 2
R = 4
LANES = 128
ROWS = 64
MESH = pl.DeviceIdType.MESH


def wall_cases(wall, walls, flip):
    cases = []
    for s in range(3):
        other = wall + (1 - s if flip else s - 1)
        cases.append((s, other, jnp.logical_and(other >= 0, other < walls)))
    return cases


def gather_kernel(chans, walls, own_ref, ext_ref, send_sem, recv_sem, local_sem):
    chan = lax.axis_index("chan")
    wall = lax.axis_index("wall")
    valid = 1 + (wall > 0).astype(jnp.int32) + (wall < walls - 1).astype(jnp.int32)
    keep = pltpu.make_async_copy(own_ref, ext_ref.at[1], local_sem)
    keep.start()
    barrier = pltpu.get_barrier_semaphore()
    for s, other, there in wall_cases(wall, walls, False):
        @pl.when(there)
        def _(s=s, other=other):
            for k in range(R + 1):
                if k == 0 and s == 1:
                    continue
                pl.semaphore_signal(
                    barrier, inc=1, device_id=(lax.rem(chan + k, chans), other), device_id_type=MESH
                )
    pl.semaphore_wait(barrier, (R + 1) * valid - 1)

    def copy(k, s, other):
        return pltpu.make_async_remote_copy(
            src_ref=own_ref,
            dst_ref=ext_ref.at[k * 3 + s],
            send_sem=send_sem.at[k * 3 + s],
            recv_sem=recv_sem.at[k * 3 + s],
            device_id=(lax.rem(chan + chans - k, chans), other),
            device_id_type=MESH,
        )

    for k in range(R, -1, -1):
        for s, other, there in wall_cases(wall, walls, True):
            if k == 0 and s == 1:
                continue

            @pl.when(there)
            def _(k=k, s=s, other=other):
                copy(k, s, other).start()

    for k in range(R + 1):
        for s, other, there in wall_cases(wall, walls, False):
            if k == 0 and s == 1:
                continue

            @pl.when(there)
            def _(k=k, s=s, other=other):
                copy(k, s, other).wait_recv()

    for k in range(R + 1):
        for s, other, there in wall_cases(wall, walls, True):
            if k == 0 and s == 1:
                continue

            @pl.when(there)
            def _(k=k, s=s, other=other):
                copy(k, s, other).wait_send()
    keep.wait()


def gather(own, chans, walls):
    slots = (R + 1) * 3
    return pl.pallas_call(
        functools.partial(gather_kernel, chans, walls),
        out_shape=jax.ShapeDtypeStruct((slots,) + own.shape, own.dtype),
        in_specs=[pl.BlockSpec(memory_space=pltpu.VMEM)],
        out_specs=pl.BlockSpec(memory_space=pl.ANY),
        scratch_shapes=[
            pltpu.SemaphoreType.DMA((slots,)),
            pltpu.SemaphoreType.DMA((slots,)),
            pltpu.SemaphoreType.DMA,
        ],
        compiler_params=pltpu.CompilerParams(collective_id=0, has_side_effects=True),
    )(own)


def pair_kernel(
    walls,
    lists_ref,
    counts_ref,
    own_ref,
    ext_ref,
    gained_ref,
    handed_ref,
    cols,
    gacc,
    gains,
    hands,
    used,
    blocks_ref,
    sem,
):
    tiles, _, tile_len = own_ref.shape
    lane_blocks = tile_len // LANES
    list_len = lists_ref.shape[0] // ((R + 1) * tiles)
    wall = lax.axis_index("wall")
    filled = jnp.zeros((ext_ref.shape[0], LANES), jnp.float32)
    for h in range(lane_blocks):
        filled += (ext_ref[:, 3, h * LANES : (h + 1) * LANES] > 0.0).astype(jnp.float32)
    used[...] = jnp.transpose(filled, (1, 0))[:8].astype(jnp.int32)
    fetch = pltpu.make_async_copy(used, blocks_ref, sem)
    fetch.start()
    hands[...] = jnp.zeros_like(hands)
    fetch.wait()

    def own_tile(t, carry):
        turned = jnp.transpose(own_ref[t], (1, 0))
        for i in range(4):
            scale = 1.0 / R if i < 3 else 1.0
            cols[i] = jnp.broadcast_to(turned[:, i : i + 1] * scale, (tile_len, LANES))
        gacc[...] = jnp.zeros_like(gacc)
        groups = (counts_ref[t] + (ROWS - 1)) // ROWS

        def partner(m, carry):
            k = m // list_len
            j = m - k * list_len
            tile = lists_ref[(k * tiles + t) * list_len + j]
            at = k * 3 * tiles + tile
            slab = tile // tiles
            edge = wall + slab - 1
            real = jnp.logical_and(edge >= 0, edge < walls)
            blocks = jnp.where(real, blocks_ref[0, at], 0)
            lift = (slab - 1).astype(jnp.float32) * 2.0
            ahead = k.astype(jnp.float32) * (1.0 / R)

            def run(width):
                row = ext_ref[at]
                lanes = [pl.ds(h * LANES, LANES) for h in range(width)]

                def spread(i, h, scale, shift):
                    value = row[i : i + 1, h * LANES : (h + 1) * LANES]
                    if scale is not None:
                        value = value * scale + shift
                    return jnp.broadcast_to(value, (8, LANES))

                theirs = [
                    (
                        spread(0, h, 1.0 / R, ahead),
                        spread(1, h, 1.0 / R, lift),
                        spread(2, h, 1.0 / R, 0.0),
                        spread(3, h, None, None),
                    )
                    for h in range(width)
                ]

                def rows(g, sums):
                    sums = list(sums)
                    base = g * ROWS
                    for r in range(0, ROWS, 8):
                        here = pl.ds(pl.multiple_of(base + r, 8), 8)
                        ax, ay, az, aw = (cols[i, here, :] for i in range(4))
                        total = None
                        for h in range(width):
                            bx, by, bz, bw = theirs[h]
                            dx, dy, dz = ax - bx, ay - by, az - bz
                            square = dx * dx + dy * dy + (dz * dz + 0.0001 / (R * R))
                            q = square * lax.rsqrt(square)
                            outer = jnp.maximum(2.0 - q, 0.0)
                            inner = jnp.maximum(1.0 - q, 0.0)
                            weight = outer * outer * outer - (inner * inner) * (inner * 4.0)
                            part = weight * bw
                            total = part if total is None else total + part
                            sums[h] = sums[h] + weight * aw
                        gacc[here, :] += total
                    return tuple(sums)

                zero = jnp.zeros((8, LANES), jnp.float32)
                sums = lax.fori_loop(0, groups, rows, (zero,) * width)
                for h in range(width):
                    hands[at, :, lanes[h]] += sums[h]

            for width in range(1, lane_blocks + 1):
                pl.when(blocks == width)(functools.partial(run, width))
            return carry

        lax.fori_loop(0, (R + 1) * list_len, partner, 0)
        gains[t] = jnp.sum(
            jnp.transpose(gacc[...], (1, 0)).reshape(LANES // 8, 8, tile_len), axis=0
        )
        return carry

    lax.fori_loop(0, tiles, own_tile, 0)
    gained_ref[...] = jnp.sum(gains[...], axis=1)
    handed_ref[...] = jnp.sum(hands[...], axis=1)


def pairs(lists, counts, own, ext, walls):
    tiles, _, tile_len = own.shape
    smem = pl.BlockSpec(memory_space=pltpu.SMEM)
    vmem = pl.BlockSpec(memory_space=pltpu.VMEM)
    return pl.pallas_call(
        functools.partial(pair_kernel, walls),
        out_shape=(
            jax.ShapeDtypeStruct((tiles, tile_len), jnp.float32),
            jax.ShapeDtypeStruct((ext.shape[0], tile_len), jnp.float32),
        ),
        in_specs=[smem, smem, vmem, vmem],
        out_specs=(vmem, vmem),
        scratch_shapes=[
            pltpu.VMEM((4, tile_len, LANES), jnp.float32),
            pltpu.VMEM((tile_len, LANES), jnp.float32),
            pltpu.VMEM((tiles, 8, tile_len), jnp.float32),
            pltpu.VMEM((ext.shape[0], 8, tile_len), jnp.float32),
            pltpu.VMEM((8, ext.shape[0]), jnp.int32),
            pltpu.SMEM((8, ext.shape[0]), jnp.int32),
            pltpu.SemaphoreType.DMA,
        ],
    )(lists, counts, own, ext)


def return_kernel(chans, walls, tiles, gained_ref, handed_ref, out_ref, held, send_sem, recv_sem):
    chan = lax.axis_index("chan")
    wall = lax.axis_index("wall")
    valid = 1 + (wall > 0).astype(jnp.int32) + (wall < walls - 1).astype(jnp.int32)
    barrier = pltpu.get_barrier_semaphore()
    for s, other, there in wall_cases(wall, walls, True):
        @pl.when(there)
        def _(s=s, other=other):
            for k in range(1, R + 1):
                pl.semaphore_signal(
                    barrier,
                    inc=1,
                    device_id=(lax.rem(chan + chans - k, chans), other),
                    device_id_type=MESH,
                )
    pl.semaphore_wait(barrier, R * valid)

    def copy(k, s, other):
        slot = (k - 1) * 3 + s
        return pltpu.make_async_remote_copy(
            src_ref=handed_ref.at[pl.ds((k * 3 + s) * tiles, tiles)],
            dst_ref=held.at[slot],
            send_sem=send_sem.at[slot],
            recv_sem=recv_sem.at[slot],
            device_id=(lax.rem(chan + k, chans), other),
            device_id_type=MESH,
        )

    for k in range(R, 0, -1):
        for s, other, there in wall_cases(wall, walls, False):
            @pl.when(there)
            def _(k=k, s=s, other=other):
                copy(k, s, other).start()

    out_ref[...] = gained_ref[...]
    for k in range(1, R + 1):
        for s, other, there in wall_cases(wall, walls, True):
            @pl.when(there)
            def _(k=k, s=s, other=other):
                copy(k, s, other).wait_recv()
                out_ref[...] += held[(k - 1) * 3 + s]

    for k in range(1, R + 1):
        for s, other, there in wall_cases(wall, walls, False):
            @pl.when(there)
            def _(k=k, s=s, other=other):
                copy(k, s, other).wait_send()


def hand_back(gained, handed, chans, walls):
    tiles, tile_len = gained.shape
    vmem = pl.BlockSpec(memory_space=pltpu.VMEM)
    return pl.pallas_call(
        functools.partial(return_kernel, chans, walls, tiles),
        out_shape=jax.ShapeDtypeStruct(gained.shape, gained.dtype),
        in_specs=[vmem, vmem],
        out_specs=vmem,
        scratch_shapes=[
            pltpu.VMEM((R * 3, tiles, tile_len), jnp.float32),
            pltpu.SemaphoreType.DMA((R * 3,)),
            pltpu.SemaphoreType.DMA((R * 3,)),
        ],
        compiler_params=pltpu.CompilerParams(collective_id=1, has_side_effects=True),
    )(gained, handed)


def on_device(chans, walls, coords, masses, counts, lists):
    tiles = counts.shape[2]
    tile_len = masses.shape[2] // tiles
    slots = jnp.arange(tile_len, dtype=jnp.int32)
    filled = (slots[None, :] < counts[0, 0][:, None]).astype(jnp.float32)
    weighted = masses.reshape(tiles, tile_len) * filled
    own = jnp.concatenate([coords.reshape(3, tiles, tile_len), weighted[None]], axis=0)
    own = jnp.moveaxis(own, 0, 1)
    ext = gather(own, chans, walls)
    gained, handed = pairs(
        lists.reshape(-1), counts.reshape(-1), own, ext.reshape(-1, 4, tile_len), walls
    )
    total = hand_back(gained, handed, chans, walls)
    scale = 1.0 / (4.0 * math.pi * NB * tile_len)
    return (total * filled * scale).reshape(1, 1, -1)


def solution(mesh):
    placed = (
        P(None, "chan", "wall", None),
        P("chan", "wall", None),
        P("chan", "wall", None),
        P("chan", "wall", None, None, None),
    )
    body = functools.partial(on_device, mesh.shape["chan"], mesh.shape["wall"])
    return jax.shard_map(
        body, mesh=mesh, in_specs=placed, out_specs=P("chan", "wall", None), check_vma=False
    )
```
